128 devices in a mesh: blk: 32 (over y, z, x_hi), tab: 4 (over x_lo, core).
Axes of the slice: x: 4 (x_hi: 2, x_lo: 2; x = x_hi * 2 + x_lo), y: 4, z: 4, core: 2. Of those that a mesh axis runs over, the one named last changes fastest.
Arguments:
- accounts: bfloat16 [262144, 128], P(('blk', 'tab')), may hold values from -0.5 to 0.5
- merchants: bfloat16 [262144, 128], P(('blk', 'tab')), may hold values from -6 to 6
- logit_scale: float32 [1], replicated, may hold values from 1 to 4
- logit_bias: float32 [1], replicated, may hold values from -3 to -1
- positive: int32 [262144], P(('blk', 'tab')), may hold values from 0 to 8191
- account_ids: int32 [262144], P(('blk', 'tab')), may hold values from 0 to 1023
- merchant_ids: int32 [262144], P(('blk', 'tab')), may hold values from 0 to 1023
- account_owner: int32 [2048, 1], P(('blk', 'tab')), may hold values from 0 to 3; in each aligned block of 16 rows (0 to 15, 16 to 31, ...) at most 8 rows name the same one
- merchant_owner: int32 [2048, 1], P(('blk', 'tab')), may hold values from 0 to 3; in each aligned block of 16 rows (0 to 15, 16 to 31, ...) at most 8 rows name the same one
Outputs:
- account_grad: float32 [131072, 128], P(('blk', 'tab'))
- merchant_grad: float32 [131072, 128], P(('blk', 'tab'))
The draws below stay inside these ranges and needn't reach their ends.
Inputs may be any that keep to these rules, and one draw needn't show every extreme that they name: `account_owner`: among the 16 row blocks of one batch block at most 8 have the same owner, and some batch block gives exactly 8 to one owner. `merchant_owner`: among the 16 row blocks of one batch block at most 8 have the same owner, and some batch block gives exactly 8 to one owner.
All inputs are finite; a program needn't handle non-finite values.
Results may differ from the reference program's by a relative error of at most 0.00048.
Values may be sent and summed in bfloat16 or wider, within the bound.
No kernel may reach another device: no remote copies, remote signals or barrier semaphores. Data moves between devices by JAX's collectives and lax.ppermute only.
A program may use at most 64 MiB of HBM per device.

```python
import math
import jax
import jax.numpy as jnp
import numpy as np
from jax import lax

D = 128
A_DEV = 2048
STEPS = 4
BLOCK_ROWS = 128
TROWS = 1024
BLOCKS_DEV = 16
CAP = 8
ROWS = 262144
N_BLK = 32
N_TAB = 4


def plant(entries, rng, low, largest):
    shape = entries.shape
    place = [jax.random.randint(jax.random.fold_in(rng, axis), (), 0, shape[axis]) for axis in range(len(shape))]
    entries = entries.at[tuple(place)].set(low)
    longest = shape.index(max(shape))
    place[longest] = (place[longest] + 1) % shape[longest]
    return entries.at[tuple(place)].set(largest)


def level_of(key, dims, cuts, low, high):
    loudness = 1.0
    for axis_at, shards_of in cuts:
        draws = jax.random.uniform(jax.random.fold_in(jax.random.fold_in(key, 6), axis_at), (shards_of,), jnp.float32, low / len(cuts), high / len(cuts))
        loudness = loudness * jnp.repeat(jnp.exp(draws), dims[axis_at] // shards_of).reshape((-1,) + (1,) * (len(dims) - 1 - axis_at))
    return loudness


def cumulative_ranks(amount, slope):
    weights = [(1 << 20) // math.isqrt(standing ** slope) + 1 for standing in range(1, amount + 1)]
    spread = 1 + sum(weights) // (1 << 30)
    return np.cumsum(np.array([max(1, weight // spread) for weight in weights]))


def ranked(rng, extent, count, lean):
    listing = cumulative_ranks(count, lean)
    pick = jax.random.randint(jax.random.fold_in(rng, 1), extent, 0, int(listing[count - 1]))
    standing = jnp.searchsorted(jnp.asarray(listing, jnp.int32), pick, side="right")
    return jax.random.permutation(jax.random.fold_in(rng, 2), count)[standing].astype(jnp.int32)


def deal_out(rng, own, number, rows, count, top, bound, skew):
    sequence = jax.random.permutation(rng, count)
    crowded, common = load_shares(count, rows * top, bound, skew, True), load_shares(count, rows * top, bound, skew, False)
    places = jnp.arange(count)

    def named(tallies, offset_by):
        used = int((tallies > 0).sum())
        fixed = max(1, used // 4)
        moved = fixed + (places - fixed + offset_by * (used - fixed)) % max(1, count - fixed)
        return jnp.zeros((count,), jnp.int32).at[sequence[jnp.where(places < fixed, places, moved)]].set(jnp.asarray(tallies, jnp.int32))

    tallies = jnp.where(number % 4 == 0, named(crowded, number // 4), named(common, number - number // 4 - 1))
    mixed = jax.random.permutation(jax.random.fold_in(own, 3), count)
    source_of, sink = mixed[0:count // 2 * 2:2], mixed[1:count // 2 * 2:2]
    room = jnp.minimum(tallies[source_of] - 1, bound - tallies[sink]) // 2
    room = jnp.where((source_of == sequence[0]) | (sink == sequence[0]) | (tallies[sink] == 0), 0, jnp.maximum(room, 0))
    moved = jax.random.randint(jax.random.fold_in(own, 4), (count // 2,), 0, 1 << 20) % (room + 1)
    tallies = tallies.at[source_of].add(-moved).at[sink].add(moved)
    items = jnp.searchsorted(jnp.cumsum(tallies), jnp.arange(rows * top), side="right").astype(jnp.int32)
    table = items.reshape(top, rows).T
    table = table[jax.random.permutation(jax.random.fold_in(own, 1), rows)]
    offset_by = jax.random.randint(jax.random.fold_in(own, 2), (rows, 1), 0, top)
    return jnp.take_along_axis(table, (jnp.arange(top)[None, :] + offset_by) % top, axis=1)


def load_shares(amount, total, bound, slope, full):
    portions = [(1 << 20) // math.isqrt(grade ** slope) + 1 for grade in range(1, amount + 1)]
    largest = bound if full else min(bound, max(-(-total // amount), total * portions[0] // sum(portions)))
    least = 1 if total - largest >= amount - 1 else 0
    holding, spare = [largest] + [least] * (amount - 1), total - largest - least * (amount - 1)
    while spare > 0:
        free = [i for i in range(1, amount) if holding[i] < largest] or [i for i in range(1, amount) if holding[i] < bound]
        pool, left = sum([portions[i] for i in free]), spare
        for i in free:
            extra = min(bound - holding[i], max(1, left * portions[i] // pool), spare)
            holding[i] = holding[i] + extra
            spare = spare - extra
    return np.array(holding)


def noise(rng, dims, deviation, most, cuts=(), held_as=jnp.bfloat16):
    drawn = deviation * jax.random.normal(rng, dims, jnp.float32)
    if cuts:
        drawn = drawn * level_of(rng, dims, cuts, -0.22, 0.18)
    return jnp.clip(drawn, -most, most).astype(held_as)


def setup_inputs(seed: int = 0) -> dict:
    streams_of = jax.random.split(jax.random.key(seed), 10)
    accounts = noise(streams_of[0], (ROWS, D), D ** -0.5, 0.5, ((0, 128),))
    merchants = noise(streams_of[1], (ROWS, D), 1.0, 6.0, ((0, 128),))
    logit_scale = jnp.clip(jnp.exp(jax.random.uniform(streams_of[2], (1,), jnp.float32, math.log(1.0), math.log(4.0))), 1.0, 4.0)
    logit_bias = jnp.clip(jax.random.uniform(streams_of[3], (1,), jnp.float32, -3.0, -1.0), -3.0, -1.0)
    positive = plant(jax.random.randint(streams_of[4], (ROWS,), 0, STEPS * A_DEV), jax.random.fold_in(streams_of[4], 1), 0, (STEPS * A_DEV) - 1).astype(jnp.int32)
    account_ids = plant(ranked(streams_of[5], (ROWS,), TROWS, 2), jax.random.fold_in(streams_of[5], 3), 0, TROWS - 1).astype(jnp.int32)
    merchant_ids = plant(ranked(streams_of[6], (ROWS,), TROWS, 2), jax.random.fold_in(streams_of[6], 3), 0, TROWS - 1).astype(jnp.int32)
    account_owner_keys = jax.random.split(jax.random.fold_in(streams_of[7], 1), (N_BLK * N_TAB * BLOCKS_DEV) // BLOCKS_DEV)
    account_owner_turns = jax.random.permutation(jax.random.fold_in(streams_of[7], 3), (N_BLK * N_TAB * BLOCKS_DEV) // BLOCKS_DEV)
    account_owner = jax.vmap(lambda own, number: deal_out(jax.random.fold_in(streams_of[7], 2), own, number, BLOCKS_DEV, N_TAB, 1, CAP, 2))(account_owner_keys, account_owner_turns).reshape((N_BLK * N_TAB * BLOCKS_DEV, 1))
    merchant_owner_keys = jax.random.split(jax.random.fold_in(streams_of[8], 1), (N_BLK * N_TAB * BLOCKS_DEV) // BLOCKS_DEV)
    merchant_owner_turns = jax.random.permutation(jax.random.fold_in(streams_of[8], 3), (N_BLK * N_TAB * BLOCKS_DEV) // BLOCKS_DEV)
    merchant_owner = jax.vmap(lambda own, number: deal_out(jax.random.fold_in(streams_of[8], 2), own, number, BLOCKS_DEV, N_TAB, 1, CAP, 2))(merchant_owner_keys, merchant_owner_turns).reshape((N_BLK * N_TAB * BLOCKS_DEV, 1))
    return {"accounts": accounts, "merchants": merchants, "logit_scale": logit_scale, "logit_bias": logit_bias, "positive": positive, "account_ids": account_ids, "merchant_ids": merchant_ids, "account_owner": account_owner, "merchant_owner": merchant_owner}


def tile_grads(acc_block, merch_block, relative, offset, scale, bias):
    row_step = min(512, A_DEV)
    count = acc_block.shape[0] // row_step
    pieces = acc_block.reshape(count, row_step, D)
    labels = relative.reshape(count, row_step)
    columns = offset + jnp.arange(merch_block.shape[0], dtype=jnp.int32)

    def one_block(carry, item):
        piece, label = item
        logits = scale * lax.dot_general(piece, merch_block, (((1,), (1,)), ((), ())), preferred_element_type=jnp.float32) + bias
        signs = jnp.where(label[:, None] == columns[None, :], jnp.float32(1.0), jnp.float32(-1.0))
        delta = (-signs * jax.nn.sigmoid(-signs * logits)).astype(jnp.bfloat16)
        grad_rows = scale * jnp.dot(delta, merch_block, preferred_element_type=jnp.float32)
        merch_part = carry + scale * lax.dot_general(delta, piece, (((0,), (0,)), ((), ())), preferred_element_type=jnp.float32)
        return merch_part, grad_rows

    start = jnp.zeros((merch_block.shape[0], D), jnp.float32)
    merch_grad, acc_grad = lax.scan(one_block, start, (pieces, labels))
    return acc_grad.reshape(-1, D), merch_grad


def table_sum(grads, ids, owner):
    devices = N_BLK * N_TAB
    owner_rows = jnp.repeat(owner.reshape(devices, A_DEV // BLOCK_ROWS), BLOCK_ROWS, axis=1).reshape(-1)
    group = jnp.repeat(jnp.arange(devices, dtype=jnp.int32) // N_TAB, A_DEV)
    target = ((group * N_TAB + owner_rows) * TROWS + ids).astype(jnp.int32)
    return jax.ops.segment_sum(grads, target, num_segments=devices * TROWS)


def reference(accounts, merchants, logit_scale, logit_bias, positive, account_ids, merchant_ids, account_owner, merchant_owner):
    devices = N_BLK * N_TAB
    scale = logit_scale[0]
    bias = logit_bias[0]
    acc_four = accounts.reshape(N_BLK, N_TAB, A_DEV, D)
    merch_four = merchants.reshape(N_BLK, N_TAB, A_DEV, D)
    labels = positive.reshape(devices, A_DEV)
    acc_total = jnp.zeros((N_BLK, N_TAB, A_DEV, D), jnp.float32)
    merch_total = jnp.zeros((N_BLK, N_TAB, A_DEV, D), jnp.float32)
    for cycle_step in range(STEPS):
        partner = jnp.roll(merch_four, cycle_step, axis=0).reshape(devices, A_DEV, D)

        def per_block(item, cycle_step=cycle_step):
            return tile_grads(item[0], item[1], item[2], cycle_step * A_DEV, scale, bias)

        acc_part, merch_part = lax.map(per_block, (acc_four.reshape(devices, A_DEV, D), partner, labels))
        acc_total = acc_total + acc_part.reshape(N_BLK, N_TAB, A_DEV, D)
        merch_total = merch_total + jnp.roll(merch_part.reshape(N_BLK, N_TAB, A_DEV, D), -cycle_step, axis=0)
    account_grad = table_sum(acc_total.reshape(-1, D), account_ids, account_owner)
    merchant_grad = table_sum(merch_total.reshape(-1, D), merchant_ids, merchant_owner)
    return account_grad, merchant_grad
```

```python
import functools

import jax
import jax.numpy as jnp
from jax import lax
from jax.experimental import pallas as pl
from jax.experimental.pallas import tpu as pltpu
from jax.sharding import PartitionSpec as P

D = 128
BLOCK_ROWS = 128
TROWS = 1024
N = 2048
BLOCKS = N // BLOCK_ROWS
TILE = 256
NT = (((1,), (1,)), ((), ()))
BASE = 64


def shifted(block, distance):
    devices = range(lax.axis_size("blk"))
    route = [((i - distance) % len(devices), i) for i in devices]
    return lax.ppermute(block, "blk", route)


def tab_swap(block, bit):
    return lax.ppermute(block, "tab", [(k, k ^ bit) for k in range(4)])


def one_pass(x, y, left, right, out, half_scale, half_bias):
    for c in range(0, N, TILE):
        cols = y[c : c + TILE, :]
        logits = lax.dot_general(x[...], cols, NT, preferred_element_type=jnp.float32)
        t = jnp.tanh(logits * half_scale + half_bias)
        parts = []
        for k in range(0, TILE, 128):
            j = (c + k) // 128
            hit = left[...] == right[j : j + 1, :]
            parts.append(t[:, k : k + 128] + jnp.where(hit, jnp.float32(-1), jnp.float32(1)))
        delta2 = jnp.concatenate(parts, axis=1).astype(jnp.bfloat16)
        out[...] += jnp.dot(delta2, cols, preferred_element_type=jnp.float32)


def lane_iota():
    shape = (BLOCKS, 128)
    return lax.broadcasted_iota(jnp.int32, shape, 0) * 128 + lax.broadcasted_iota(jnp.int32, shape, 1)


def row_iota():
    return lax.broadcasted_iota(jnp.int32, (N, 128), 0)


def guest_labels(guest, step):
    high = guest[N : N + BLOCKS, :].astype(jnp.float32)
    low = guest[N + BLOCKS : N + 2 * BLOCKS, :].astype(jnp.float32)
    return (high * BASE + low).astype(jnp.int32) - step * N


def both_passes(xs, ys, left, right, out, half_scale, half_bias):
    def body(p, carry):
        one_pass(xs.at[p], ys.at[p], left.at[p], right.at[p], out.at[p], half_scale, half_bias)
        return carry

    lax.fori_loop(0, 2, body, 0)


def own_kernel(coef, acc, merch, labels, out, label_rows, xs, ys, left, right):
    for j in range(BLOCKS):
        block = jnp.broadcast_to(labels[j : j + 1, :], (128, 128))
        label_rows[j * 128 : (j + 1) * 128, :] = block.T
    xs[0] = acc[...]
    ys[0] = merch[...]
    xs[1] = merch[...]
    ys[1] = acc[...]
    left[0] = label_rows[...]
    left[1] = row_iota()
    right[0] = lane_iota()
    right[1] = labels[...]
    out[...] = jnp.zeros_like(out)
    both_passes(xs, ys, left, right, out, coef[0], coef[1])


def step_kernel(coef, acc, merch, visiting, guest, label_rows, prev, out, xs, ys, left, right, *, step):
    xs[0] = acc[...]
    ys[0] = visiting[...]
    xs[1] = merch[...]
    ys[1] = guest[0:N, :]
    left[0] = label_rows[...] - step * N
    left[1] = row_iota()
    right[0] = lane_iota()
    right[1] = guest_labels(guest, step)
    out[...] = prev[...]
    both_passes(xs, ys, left, right, out, coef[0], coef[1])


def scatter_blocks(grad, scale, ids, owner, here, table, keep, send):
    table[...] = jnp.zeros_like(table)
    target_rows = lax.broadcasted_iota(jnp.int32, (TROWS, 128), 0)

    def body(j, carry):
        first = pl.multiple_of(j * BLOCK_ROWS, BLOCK_ROWS)
        rows = grad[pl.ds(first, BLOCK_ROWS), :] * scale
        high = rows.astype(jnp.bfloat16)
        low = (rows - high.astype(jnp.float32)).astype(jnp.bfloat16)
        pair = jnp.concatenate([high, low], axis=1)
        hot = jnp.where(target_rows == ids[pl.ds(j, 1), :], jnp.float32(1), jnp.float32(0)).astype(jnp.bfloat16)
        both = jnp.dot(hot, pair, preferred_element_type=jnp.float32)
        slot = (owner[j] ^ here) & 3
        place = pl.multiple_of((slot // 2 + (slot % 2) * 2) * TROWS, TROWS)
        table[pl.ds(place, TROWS), :] += both[:, :D] + both[:, D:]
        return carry

    lax.fori_loop(0, BLOCKS, body, 0, unroll=4)
    keep[...] = table[0 : 2 * TROWS, :].reshape(2, TROWS, D)
    send[...] = table[2 * TROWS : 4 * TROWS, :].reshape(2, TROWS, D)


def last_account_kernel(coef, owner, here, acc, visiting, label_rows, prev, ids, keep, send, out, left, right, table):
    left[...] = label_rows[...] - 3 * N
    right[...] = lane_iota()
    out[...] = prev[0]
    one_pass(acc, visiting, left, right, out, coef[0], coef[1])
    scatter_blocks(out, coef[0], ids, owner, here[0], table, keep, send)


def last_merchant_kernel(coef, owner, here, merch, guest, prev, ids, keep, send, out, left, right, table):
    left[...] = row_iota()
    right[...] = guest_labels(guest, 3)
    out[...] = prev[1]
    one_pass(merch, guest, left, right, out, coef[0], coef[1])
    scatter_blocks(out, coef[0], ids, owner, here[0], table, keep, send)


def call(kernel, smem, vmem, out_shape, scratch, flops, alias=None):
    in_specs = [pl.BlockSpec(memory_space=pltpu.SMEM)] * smem + [pl.BlockSpec(memory_space=pltpu.VMEM)] * vmem
    out_specs = jax.tree.map(lambda _: pl.BlockSpec(memory_space=pltpu.VMEM), out_shape)
    return pl.pallas_call(
        kernel,
        in_specs=in_specs,
        out_specs=out_specs,
        out_shape=out_shape,
        scratch_shapes=scratch,
        input_output_aliases=alias or {},
        cost_estimate=pl.CostEstimate(flops=flops, bytes_accessed=4 << 20, transcendentals=0),
        compiler_params=pltpu.CompilerParams(vmem_limit_bytes=36 << 20),
    )


GRADS = pltpu.VMEM((2, N, D), jnp.float32)
LABELS = pltpu.VMEM((N, 128), jnp.int32)
TABLES = jax.ShapeDtypeStruct((2, TROWS, D), jnp.float32)
PAIR_SCRATCH = [
    pltpu.VMEM((2, N, D), jnp.bfloat16),
    pltpu.VMEM((2, N, D), jnp.bfloat16),
    pltpu.VMEM((2, N, 128), jnp.int32),
    pltpu.VMEM((2, BLOCKS, 128), jnp.int32),
]
LAST_SCRATCH = [
    pltpu.VMEM((N, D), jnp.float32),
    pltpu.VMEM((N, 128), jnp.int32),
    pltpu.VMEM((BLOCKS, 128), jnp.int32),
    pltpu.VMEM((4 * TROWS, D), jnp.float32),
]


PASS = 3 << 30


def in_vmem(block):
    return pltpu.with_memory_space_constraint(block, pltpu.VMEM)


def exchange(keep, send):
    both = keep + tab_swap(send, 1)
    return both[0] + tab_swap(both[1], 2)


def per_device(
    accounts,
    merchants,
    logit_scale,
    logit_bias,
    positive,
    account_ids,
    merchant_ids,
    account_owner,
    merchant_owner,
):
    coef = 0.5 * jnp.concatenate([logit_scale, logit_bias])
    here = lax.axis_index("tab").astype(jnp.int32).reshape(1)
    labels = positive.reshape(BLOCKS, 128)
    digits = jnp.concatenate([labels // BASE, labels % BASE], axis=0).astype(jnp.bfloat16)
    guests = jnp.concatenate([accounts, digits], axis=0)

    visiting2 = shifted(merchants, 2)
    visiting1 = shifted(merchants, 1)
    guest2 = shifted(guests, -2)
    guest1 = shifted(guests, -1)

    grads, label_rows = call(own_kernel, 1, 3, [GRADS, LABELS], PAIR_SCRATCH, 2 * PASS)(
        coef, accounts, merchants, labels
    )
    grads = call(functools.partial(step_kernel, step=2), 1, 6, GRADS, PAIR_SCRATCH, 2 * PASS, {6: 0})(
        coef, accounts, merchants, visiting2, guest2, in_vmem(label_rows), in_vmem(grads)
    )
    visiting1, guest1, grads = lax.optimization_barrier((visiting1, guest1, grads))
    visiting3 = shifted(visiting1, 2)
    guest3 = shifted(guest1, -2)
    grads = call(functools.partial(step_kernel, step=1), 1, 6, GRADS, PAIR_SCRATCH, 2 * PASS, {6: 0})(
        coef, accounts, merchants, visiting1, guest1, in_vmem(label_rows), in_vmem(grads)
    )
    visiting3, guest3, grads = lax.optimization_barrier((visiting3, guest3, grads))
    keep, send = call(last_account_kernel, 3, 5, [TABLES, TABLES], LAST_SCRATCH, 2 * PASS)(
        coef, account_owner[:, 0], here, accounts, visiting3, in_vmem(label_rows), in_vmem(grads), account_ids.reshape(BLOCKS, 128)
    )
    account_grad = exchange(keep, send)
    keep, send = call(last_merchant_kernel, 3, 4, [TABLES, TABLES], LAST_SCRATCH, 2 * PASS)(
        coef, merchant_owner[:, 0], here, merchants, guest3, in_vmem(grads), merchant_ids.reshape(BLOCKS, 128)
    )
    merchant_grad = exchange(keep, send)
    return (account_grad, merchant_grad)


def solution(mesh):
    return jax.shard_map(
        per_device,
        mesh=mesh,
        in_specs=(
            P(("blk", "tab"), None),
            P(("blk", "tab"), None),
            P(),
            P(),
            P(("blk", "tab")),
            P(("blk", "tab")),
            P(("blk", "tab")),
            P(("blk", "tab"), None),
            P(("blk", "tab"), None),
        ),
        out_specs=(P(("blk", "tab"), None), P(("blk", "tab"), None)),
        check_vma=False,
    )
```
